32 devices in a mesh: grp: 4 (over z), row: 8 (over y, x, core).
Axes of the slice: x: 2, y: 2, z: 4, core: 2. Of those that a mesh axis runs over, the one named last changes fastest.
Arguments:
- probes: bfloat16 [4, 8192, 2048], P('grp', 'row'), may hold values from -6 to 6
- solves: bfloat16 [4, 8192, 2048], P('grp', 'row'), may hold values from -6 to 6
- row_spectra: float32 [8, 8192], replicated, may hold values from -0.0625 to 0.0625
- col_spectra: float32 [8, 2048], replicated, may hold values from -0.125 to 0.125
Outputs:
- row_traces: float32 [8, 8192], P(None, ('grp', 'row'))
- col_traces: float32 [8, 2048], replicated
The draws below stay inside these ranges and needn't reach their ends.
All inputs are finite; a program needn't handle non-finite values.
Results may differ from the reference program's by a relative error of at most 0.0003.
Values sent between devices are 32-bit elements; how exact they have to be, the bound alone decides.
No kernel may reach another device: no remote copies, remote signals or barrier semaphores. Data moves between devices by JAX's collectives and lax.ppermute only.
A program may use at most 128 MiB of HBM per device.

```python
import jax
import jax.numpy as jnp
from jax import lax

L1 = 8192
L2 = 2048
HYPER = 8
PROBES = 4


def block_scale(key, extent, cuts, least, largest):
    factor_of, own = 1.0, jax.random.fold_in(key, 6)
    for position, shards_of in cuts:
        draws = jnp.exp(jax.random.uniform(jax.random.fold_in(own, position), (shards_of,), jnp.float32, least / len(cuts), largest / len(cuts)))
        factor_of = factor_of * jnp.repeat(draws, extent[position] // shards_of).reshape([-1 if axis == position else 1 for axis in range(len(extent))])
    return factor_of


def centred(rng, shape, spread, reach, pieces=(), kind=jnp.bfloat16):
    gain = block_scale(rng, shape, pieces, -0.22, 0.18) if pieces else 1.0
    values = jax.random.normal(rng, shape, jnp.float32) * spread * gain
    return jnp.minimum(jnp.maximum(values, -reach), reach).astype(kind)


def setup_inputs(seed: int = 0) -> dict:
    arg_keys = jax.random.split(jax.random.key(seed), 5)
    return {
        "probes": centred(arg_keys[0], (PROBES, L1, L2), 1.0, 6.0, ((0, 4), (1, 8))),
        "solves": centred(arg_keys[1], (PROBES, L1, L2), 1.0, 6.0, ((0, 4), (1, 8))),
        "row_spectra": centred(arg_keys[2], (HYPER, L1), L1 ** -0.5, 0.0625, (), jnp.float32),
        "col_spectra": centred(arg_keys[3], (HYPER, L2), L2 ** -0.5, 0.125, (), jnp.float32),
    }


def reference(probes, solves, row_spectra, col_spectra):
    def one_probe(total, pair):
        zhat = jnp.fft.fft2(pair[0].astype(jnp.float32))
        uhat = jnp.fft.fft2(pair[1].astype(jnp.float32))
        term = jnp.real(zhat) * jnp.real(uhat) + jnp.imag(zhat) * jnp.imag(uhat)
        return total + term.astype(total.dtype), None

    start_total = jnp.zeros((L1, L2), jnp.float32)
    total, _ = lax.scan(one_probe, start_total, (probes, solves))
    cross = total / (PROBES * L1 * L2)
    row_traces = jnp.einsum("kj,ij->ki", col_spectra, cross, precision=lax.Precision.HIGHEST)
    col_traces = jnp.einsum("ki,ij->kj", row_spectra, cross, precision=lax.Precision.HIGHEST)
    return row_traces, col_traces
```

```python
import functools
import math

import jax
import jax.numpy as jnp
import numpy as np
from jax import lax
from jax.experimental import pallas as pl
from jax.experimental.pallas import tpu as pltpu
from jax.sharding import PartitionSpec as P

LANES = 128
COLS = 64
INNER = 128
FINE = 64
TILE = 16
GROUP = 8
VMEM_LIMIT = 60 * 1024 * 1024


matmul = functools.partial(jnp.dot, preferred_element_type=jnp.float32)


def split(x):
    high = x.astype(jnp.bfloat16)
    return high, (x - high.astype(jnp.float32)).astype(jnp.bfloat16)


def split_plain(x):
    high = lax.reduce_precision(x, 8, 7)
    return high.astype(jnp.bfloat16), (x - high).astype(jnp.bfloat16)


def column_tables(second_len, shards, chunks):
    half = second_len // 2
    j = (
        np.arange(shards)[None, :, None] * (half // shards)
        + np.arange(chunks)[:, None, None] * COLS
        + np.arange(COLS)
    )
    freq = np.stack([j, np.where(j == 0, half, j)], axis=2).reshape(chunks, 1, -1)
    turn = np.stack([np.zeros(j.shape), np.where(j == 0, 0.0, 0.5 * math.pi)], axis=2).reshape(chunks, 1, -1)
    unit = 2.0 * math.pi / second_len
    coarse = np.arange(second_len // FINE)[None, :, None] * FINE
    big = (coarse * freq % second_len) * unit + turn
    small = (np.arange(FINE)[None, :, None] * freq % second_len) * unit
    return [t.astype(np.float32) for t in (np.cos(big), np.sin(big), np.cos(small), np.sin(small))]


def pieces_of(chunk):
    return (48, INNER - 48) if chunk == 0 else (INNER - 32, 32)


def inner_table(spans):
    k = np.arange(INNER)
    phase = (k[:, None] * k[None, :] % INNER) * (2.0 * math.pi / INNER)
    cos, sin = np.cos(phase), np.sin(phase)
    parts, at = [], 0
    for span in spans:
        c, s = cos[:, at : at + span], sin[:, at : at + span]
        parts += [np.concatenate([c, -s]), np.concatenate([s, c])]
        at += span
    table = np.concatenate(parts, axis=1).astype(np.float32)
    high = table.astype(jnp.bfloat16)
    return high, (table - high.astype(np.float32)).astype(jnp.bfloat16)


def rotate(x, count, size, sign):
    re, im = x
    count = (count * sign) % size
    if count == 0:
        return re, im
    if 4 * count == size:
        return -im, re
    if 2 * count == size:
        return -re, -im
    if 4 * count == 3 * size:
        return im, -re
    cos, sin = math.cos(2 * math.pi * count / size), math.sin(2 * math.pi * count / size)
    if (8 * count) % size == 0:
        c, s = (1 if cos > 0 else -1), (1 if sin > 0 else -1)
        root = math.sqrt(0.5)
        return (c * root) * (re - im if c == s else re + im), (s * root) * (re + im if c == s else re - im)
    return re * cos - im * sin, re * sin + im * cos


def small_fft(xs, sign):
    n = len(xs)
    if n == 1:
        return xs
    even, odd = small_fft(xs[0::2], sign), small_fft(xs[1::2], sign)
    first, second = [], []
    for k in range(n // 2):
        (er, ei), (tr, ti) = even[k], rotate(odd[k], k, n, sign)
        first.append((er + tr, ei + ti))
        second.append((er - tr, ei - ti))
    return first + second


def columns_kernel(pos_ref, p_ref, s_ref, cb_ref, sb_ref, cs_ref, ss_ref, *refs):
    outs, (high_ref, low_ref) = refs[:-2], refs[-2:]
    shards = len(outs)

    @pl.when(pl.program_id(0) == 0)
    def _():
        for m in range(shards):
            target = lax.rem(pos_ref[0] + m, shards)
            lanes = pl.ds(pl.multiple_of(target * LANES, LANES), LANES)
            cos, sin = cs_ref[:, lanes], ss_ref[:, lanes]

            @pl.loop(0, cb_ref.shape[0], unroll=4)
            def _(b, m=m, lanes=lanes, cos=cos, sin=sin):
                rows = pl.ds(pl.multiple_of(b * FINE, FINE), FINE)
                high, low = split(cb_ref[b, :, lanes] * cos - sb_ref[b, :, lanes] * sin)
                high_ref[rows, m * LANES : (m + 1) * LANES] = high
                low_ref[rows, m * LANES : (m + 1) * LANES] = low

    shape = outs[0].shape[1:]
    rows = shape[0] * shape[1]
    p = p_ref[...].reshape(rows, p_ref.shape[2])
    s = s_ref[...].reshape(rows, s_ref.shape[2])
    lower = lax.broadcasted_iota(jnp.int32, (rows, LANES), 1) < COLS
    wide = 2 * LANES
    for pair in range(shards // 2):
        at = slice(pair * wide, (pair + 1) * wide)
        first = matmul(p, high_ref[:, at]) + matmul(p, low_ref[:, at])
        second = matmul(s, high_ref[:, at]) + matmul(s, low_ref[:, at])
        for m in range(2):
            a, b = first[:, m * LANES : (m + 1) * LANES], second[:, m * LANES : (m + 1) * LANES]
            out = outs[2 * pair + m]
            out[0] = jnp.where(lower, a, pltpu.roll(b, COLS, 1)).reshape(shape)
            out[1] = jnp.where(lower, pltpu.roll(a, COLS, 1), b).reshape(shape)


def columns(p, s, tables, position, shards, begin, span):
    rows, second_len = p.shape
    depth = rows // INNER
    per_step = max(1, depth // 2)
    lanes = tables[0].shape[-1]
    tables = [t[:, None] if n < 2 else t for n, t in enumerate(tables)]
    p, s = (x.reshape(depth, INNER, second_len) for x in (p, s))
    whole = lambda a: pl.BlockSpec(a.shape, lambda i, pos: (0,) * a.ndim)
    return pl.pallas_call(
        columns_kernel,
        grid_spec=pltpu.PrefetchScalarGridSpec(
            num_scalar_prefetch=1,
            grid=(depth // per_step,),
            in_specs=[
                pl.BlockSpec(
                    (pl.Element(per_step), pl.Element(span), pl.Element(second_len)),
                    lambda i, pos: (i * per_step, begin, 0),
                )
            ]
            * 2
            + [whole(t) for t in tables],
            out_specs=[pl.BlockSpec((2, per_step, span, LANES), lambda i, pos: (0, i, 0, 0))] * shards,
            scratch_shapes=[pltpu.VMEM((second_len, lanes), jnp.bfloat16)] * 2,
        ),
        out_shape=[jax.ShapeDtypeStruct((2, depth, span, LANES), jnp.float32)] * shards,
        compiler_params=pltpu.CompilerParams(vmem_limit_bytes=VMEM_LIMIT),
        cost_estimate=pl.CostEstimate(
            flops=8 * depth * span * second_len * lanes,
            bytes_accessed=4 * depth * span * second_len + 8 * shards * depth * span * LANES,
            transcendentals=0,
        ),
        name="columns",
    )(position, p, s, *tables)


def outer_tile(edge, inputs, rows, turns, tmp_ref, store):
    shards, depth = len(inputs), inputs[0].shape[1]
    outer = shards * depth
    lane = lax.broadcasted_iota(jnp.int32, (TILE, LANES), 1) % COLS
    for g in range(depth):
        xs = []
        for ref in inputs:
            re, im = ref[0, g, rows], ref[1, g, rows]
            if edge:
                re = jnp.where(lane == 0, re, jnp.where(lane == 1, pltpu.roll(im, 1, 1), 0.0))
                im = jnp.zeros_like(re)
            xs.append((re, im))
        for q, y in enumerate(small_fft(xs, 1)):
            tmp_ref[q, 0, g], tmp_ref[q, 1, g] = rotate(y, g * q, outer, -1)
    for q in range(shards):
        zs = small_fft([(tmp_ref[q, 0, g], tmp_ref[q, 1, g]) for g in range(depth)], -1)
        for r, (re, im) in enumerate(zs):
            k = q + shards * r
            cos = jnp.broadcast_to(turns[:, k : k + 1], (TILE, LANES))
            sin = jnp.broadcast_to(turns[:, outer + k : outer + k + 1], (TILE, LANES))
            store(k, 0, *split(re * cos - im * sin))
            store(k, 1, *split(re * sin + im * cos))


def outer_kernel(edge, begin, *refs):
    turn_ref, high_ref, low_ref, tmp_ref = refs[-4:]
    inputs = refs[:-4]
    span = inputs[0].shape[2]

    @pl.loop(0, span // TILE)
    def _(t):
        rows = pl.ds(pl.multiple_of(t * TILE, TILE), TILE)

        def store(k, plane, high, low):
            high_ref[k, plane, rows, :] = high
            low_ref[k, plane, rows, :] = low

        first = pl.multiple_of(begin + pl.program_id(0) * span + t * TILE, TILE)
        outer_tile(edge, inputs, rows, turn_ref[pl.ds(first, TILE), :], tmp_ref, store)


def outer_stage(pieces, turns, begin, edge):
    shards = len(pieces)
    _, depth, span, _ = pieces[0].shape
    outer = shards * depth
    steps = next(n for n in (3, 2, 1) if span % (n * TILE) == 0)
    rows = span // steps
    return pl.pallas_call(
        functools.partial(outer_kernel, edge, begin),
        grid=(steps,),
        in_specs=[pl.BlockSpec((2, depth, rows, LANES), lambda i: (0, 0, i, 0))] * shards
        + [pl.BlockSpec(turns.shape, lambda i: (0, 0))],
        out_specs=[pl.BlockSpec((outer, 2, rows, LANES), lambda i: (0, 0, i, 0))] * 2,
        out_shape=[jax.ShapeDtypeStruct((outer, 2, span, LANES), jnp.bfloat16)] * 2,
        scratch_shapes=[pltpu.VMEM((shards, 2, depth, TILE, LANES), jnp.float32)],
        compiler_params=pltpu.CompilerParams(vmem_limit_bytes=VMEM_LIMIT),
        cost_estimate=pl.CostEstimate(
            flops=200 * outer * span * LANES, bytes_accessed=16 * outer * span * LANES, transcendentals=0
        ),
        name="outer",
    )(*pieces, turns)


def three_terms(x):
    high = x.astype(jnp.bfloat16)
    middle, low = split(x - high.astype(jnp.float32))
    return high, middle, low


def inner_kernel(shards, begin, edge, members, *refs):
    last = members > 0
    inputs, refs = refs[:shards], refs[shards:]
    turn_ref, prev_high, prev_low, th_ref, tl_ref, rr_ref, cw_ref, in_ref = refs[:8]
    refs = refs[8:]
    if last:
        ahead_ref, behind_ref, before_ref, keep_ref, pay_ref, acc_ref, fin_ref = refs[:7]
        refs = refs[7:]
    else:
        acc_ref, col_ref = refs[:2]
        refs = refs[2:]
    high_ref, low_ref, tmp_ref, sum_ref, sems = refs
    hypers = cw_ref.shape[1] // (2 * GROUP)
    early = prev_high.shape[1]
    copies = [
        pltpu.make_async_copy(prev, ref.at[:, pl.ds(0, early), :], sems.at[n])
        for n, (prev, ref) in enumerate(((prev_high, high_ref), (prev_low, low_ref)))
    ]
    for copy in copies:
        copy.start()
    span = inputs[0].shape[2]

    @pl.loop(0, span // TILE)
    def _(t):
        rows = pl.ds(pl.multiple_of(t * TILE, TILE), TILE)

        def store(k, plane, high, low):
            at = pl.ds(pl.multiple_of(early + plane * span + t * TILE, TILE), TILE)
            high_ref[k, at, :] = high
            low_ref[k, at, :] = low

        first = pl.multiple_of(begin + t * TILE, TILE)
        outer_tile(edge, inputs, rows, turn_ref[pl.ds(first, TILE), :], tmp_ref, store)

    for copy in copies:
        copy.wait()
    lower = lax.broadcasted_iota(jnp.int32, (INNER, LANES), 1) < COLS
    sum_ref[...] = jnp.zeros_like(sum_ref)

    @pl.loop(0, acc_ref.shape[0])
    def _(step):
        total = in_ref[step]
        part = 0.0
        for quad in range(GROUP // 4):
            xs = []
            for pair in range(2):
                k = GROUP * step + 4 * quad + 2 * pair
                high = jnp.concatenate([high_ref[k], high_ref[k + 1]], axis=1)
                low = jnp.concatenate([low_ref[k], low_ref[k + 1]], axis=1)
                out = matmul(th_ref[...], high) + matmul(th_ref[...], low) + matmul(tl_ref[...], high)
                x = 0.0
                for plane in range(2):
                    z = out[plane * INNER : (plane + 1) * INNER]
                    a, b = z[:, :LANES], z[:, LANES:]
                    x += jnp.where(lower, a, b) * pltpu.roll(jnp.where(lower, b, a), COLS, 1)
                xs.append(jnp.concatenate(split(x), axis=1))
                r = matmul(xs[-1], cw_ref[...])
                r = r[:, :LANES] + r[:, LANES:]
                turn = 2 * hypers * (2 * quad + pair)
                total += pltpu.roll(r, turn, 1) if turn else r
            part += matmul(rr_ref[GROUP // 4 * step + quad], jnp.concatenate(xs, axis=0))
        sum_ref[...] += part
        acc_ref[step] = total

    t = sum_ref[...]
    both = []
    for n in range(2):
        at = 2 * n * hypers
        both.append(
            t[at : at + hypers, :LANES] + t[at + hypers : at + 2 * hypers, :LANES] + t[at : at + hypers, LANES:]
        )
    col = both[0] + pltpu.roll(both[1], COLS, 1)
    if not last:
        col_ref[...] = col
        return

    outer = fin_ref.shape[1] * 2 // hypers
    acc = jnp.concatenate([acc_ref[n] for n in range(acc_ref.shape[0])], axis=1)
    parts = three_terms(acc)
    ahead = sum(matmul(part, ahead_ref[...]) for part in parts)
    behind = sum(matmul(part, behind_ref[...]) for part in parts)
    column = lax.broadcasted_iota(jnp.int32, behind.shape, 1)
    behind = jnp.where(column % outer == 0, pltpu.roll(behind, INNER - 1, 0), behind)
    row = lax.broadcasted_iota(jnp.int32, (INNER, INNER), 0)
    column = lax.broadcasted_iota(jnp.int32, (INNER, INNER), 1)
    flip = jnp.where(row + column == INNER - 1, 1.0, 0.0).astype(jnp.bfloat16)
    fin_ref[...] = ahead + sum(matmul(flip, part) for part in three_terms(behind))

    mine = before_ref[...] + keep_ref[0] * col + keep_ref[1] * pltpu.roll(col, COLS, 1)
    depth = INNER // members
    groups = fin_ref.shape[1] // LANES
    for d in range(members):
        for n in range(groups):
            pay_ref[d, n * depth : (n + 1) * depth, :] = fin_ref[
                d * depth : (d + 1) * depth, n * LANES : (n + 1) * LANES
            ]
        pay_ref[d, groups * depth :, :] = mine


def inner_stage(pieces, turns, begin, edge, early, table, rr, cw, acc, closing):
    shards = len(pieces)
    _, depth, span, _ = pieces[0].shape
    outer = shards * depth
    hypers = 2 * LANES // (2 * GROUP)
    early = [f.reshape(outer, -1, LANES) for f in early]
    whole = lambda a: pl.BlockSpec(a.shape, lambda i: (0,) * len(a.shape))
    scratch = []
    members = 0
    if closing:
        orders, before, keep, members = closing
        extra = [*orders, before, keep]
        lines = hypers // 2 * outer // LANES * (INNER // members) + hypers
        out_shape = [jax.ShapeDtypeStruct((members, lines, LANES), jnp.float32)]
        scratch = [pltpu.VMEM(acc.shape, jnp.float32), pltpu.VMEM((INNER, hypers // 2 * outer), jnp.float32)]
    else:
        extra = []
        out_shape = [
            jax.ShapeDtypeStruct(acc.shape, jnp.float32),
            jax.ShapeDtypeStruct((hypers, LANES), jnp.float32),
        ]
    return pl.pallas_call(
        functools.partial(inner_kernel, shards, begin, edge, members),
        grid=(1,),
        in_specs=[whole(a) for a in (*pieces, turns)]
        + [pl.BlockSpec(memory_space=pl.ANY)] * 2
        + [whole(a) for a in (*table, rr, cw, acc, *extra)],
        out_specs=[whole(a) for a in out_shape],
        out_shape=out_shape,
        scratch_shapes=scratch
        + [
            pltpu.VMEM((outer, 2 * INNER, LANES), jnp.bfloat16),
            pltpu.VMEM((outer, 2 * INNER, LANES), jnp.bfloat16),
            pltpu.VMEM((shards, 2, depth, TILE, LANES), jnp.float32),
            pltpu.VMEM((4 * hypers, 2 * LANES), jnp.float32),
            pltpu.SemaphoreType.DMA((2,)),
        ],
        compiler_params=pltpu.CompilerParams(vmem_limit_bytes=VMEM_LIMIT),
        cost_estimate=pl.CostEstimate(
            flops=2 * 3 * 4 * outer * INNER * INNER * LANES,
            bytes_accessed=8 * outer * INNER * LANES,
            transcendentals=0,
        ),
        name="inner",
    )(*pieces, turns, *early, *table, rr, cw, acc, *extra)


def orders_kernel(ahead_ref, behind_ref):
    lanes, width = ahead_ref.shape
    hypers = LANES // GROUP
    outer = lanes // hypers
    row = lax.broadcasted_iota(jnp.int32, (lanes, width), 0)
    column = lax.broadcasted_iota(jnp.int32, (lanes, width), 1)
    k, h = column % outer, column // outer
    one = lambda hit: jnp.where(hit, 1.0, 0.0).astype(jnp.bfloat16)
    ahead_ref[...] = one(row == hypers * k + h)
    behind_ref[...] = one(row == hypers * ((outer - k) % outer) + hypers // 2 + h)


def output_orders(outer, hyper):
    shape = jax.ShapeDtypeStruct((2 * hyper * outer, hyper * outer), jnp.bfloat16)
    return pl.pallas_call(
        orders_kernel,
        out_shape=[shape, shape],
        compiler_params=pltpu.CompilerParams(vmem_limit_bytes=VMEM_LIMIT),
        cost_estimate=pl.CostEstimate(flops=0, bytes_accessed=4 * shape.size, transcendentals=0),
        name="orders",
    )()


def local(probes, solves, row_spectra, col_spectra):
    shards = lax.axis_size("row")
    groups = lax.axis_size("grp")
    position = lax.axis_index("row")
    local_probes, rows, second_len = probes.shape
    hyper, first_len = row_spectra.shape
    half_len = second_len // 2
    block = half_len // shards
    chunks = block // COLS
    outer = first_len // INNER
    scale = 1.0 / (local_probes * groups * first_len * second_len)

    tables = column_tables(second_len, shards, chunks)
    where_am_i = position.astype(jnp.int32).reshape(1)

    k = jnp.arange(outer, dtype=jnp.int32)
    count = k[:, None] * jnp.arange(INNER, dtype=jnp.int32)[None, :] + (k % shards * position * rows)[:, None]
    phase = (count % first_len).astype(jnp.float32) * (2.0 * math.pi / first_len)
    turns = jnp.concatenate([jnp.cos(phase), -jnp.sin(phase)], axis=0).T

    forward = row_spectra.reshape(hyper, INNER, outer).transpose(0, 2, 1) * scale
    i = np.arange(INNER)
    exact = functools.partial(jnp.einsum, precision=lax.Precision.HIGHEST)
    turned = exact("mn,hnk->hmk", np.eye(outer, dtype=np.float32)[-np.arange(outer) % outer], forward)
    mirror = jnp.concatenate(
        [
            exact("hmk,ka->hma", turned[:, :1], np.eye(INNER, dtype=np.float32)[-i % INNER]),
            exact("hmk,ka->hma", turned[:, 1:], np.eye(INNER, dtype=np.float32)[INNER - 1 - i]),
        ],
        axis=1,
    )
    rr = jnp.concatenate([forward, mirror], axis=0)
    rr = rr.reshape(2 * hyper, outer // 4, 2, 2, INNER).transpose(1, 3, 0, 2, 4)
    rr = jnp.stack(split_plain(rr), axis=2).reshape(outer // 4, 8 * hyper, 2 * INNER)

    start = position * block
    ahead = lax.dynamic_slice_in_dim(col_spectra, start, block, 1)
    reverse = jnp.concatenate(
        [col_spectra[:, half_len : half_len + 1], col_spectra[:, :half_len:-1]], axis=1
    )
    behind = lax.dynamic_slice_in_dim(reverse, start, block, 1)
    edge_column = jnp.logical_and(position == 0, jnp.arange(block) == 0)
    both = jnp.concatenate([ahead, behind], axis=0) * scale
    main = jnp.where(edge_column, 0.0, both).reshape(2 * hyper, chunks, COLS).transpose(1, 2, 0)
    rim = jnp.where(position == 0, both[:, 0].reshape(2, hyper), 0.0)
    rim = jnp.pad(rim, ((0, COLS - 2), (0, hyper)))
    cw = jnp.concatenate([main, rim[None]], axis=0)
    cw = jnp.concatenate(
        [
            jnp.pad(cw, ((0, 0), (0, 0), (0, LANES - 2 * hyper))),
            jnp.pad(cw, ((0, 0), (0, 0), (2 * hyper, LANES - 4 * hyper))),
        ],
        axis=1,
    )
    high, low = split_plain(cw)
    cw = jnp.concatenate(
        [jnp.concatenate([high, low], axis=2), jnp.concatenate([high, jnp.zeros_like(low)], axis=2)], axis=1
    )
    orders = output_orders(outer, hyper)

    members = groups * shards
    moved = []
    for n in range(local_probes):
        for c in range(chunks):
            begin = 0
            for span in pieces_of(c):
                sent = columns(probes[n], solves[n], [t[c] for t in tables], where_am_i, shards, begin, span)
                got = [
                    lax.ppermute(sent[m], "row", [(i, (i + m) % shards) for i in range(shards)])
                    for m in range(1, shards)
                ]
                moved.append([sent[0]] + got)
                begin += span
    acc = jnp.zeros((outer // GROUP, INNER, LANES), jnp.float32)
    col_parts = [0.0] * chunks
    rim_col = 0.0
    slots = np.arange(LANES)
    for n in range(local_probes):
        for c in range(chunks):
            spans = pieces_of(c)
            table = inner_table(spans)
            (first, second), moved = moved[:2], moved[2:]
            for edge in (True, False) if c == 0 else (False,):
                early = outer_stage(first, turns, 0, edge)
                closing = None
                if n == local_probes - 1 and c == chunks - 1 and not edge:
                    rim_first = jnp.concatenate([rim_col[:hyper, 0], rim_col[:hyper, 1]])[:, None]
                    rim_first = jnp.where(jnp.logical_and(position == 0, slots == 0), rim_first, 0.0)
                    clear = jnp.where(jnp.logical_and(position == 0, slots == 0), 0.0, 1.0)
                    mine = jnp.pad(
                        jnp.concatenate(
                            [jnp.zeros((2 * hyper, 0), jnp.float32)]
                            + [
                                jnp.broadcast_to(part, (2 * hyper, LANES))[:, :COLS] + jnp.zeros((2 * hyper, COLS))
                                for part in col_parts
                            ],
                            axis=1,
                        ),
                        ((0, 0), (0, LANES - chunks * COLS)),
                    )
                    before = mine * clear + rim_first
                    keep = jnp.stack(
                        [jnp.where((slots // COLS == c) & (c == k), clear, 0.0) for k in range(2)]
                    )
                    keep = jnp.broadcast_to(keep[:, None], (2, 2 * hyper, LANES))
                    closing = (orders, before, keep, members)
                out = inner_stage(
                    second, turns, spans[0], edge, early, table, rr, cw[chunks if edge else c], acc, closing
                )
                if closing:
                    (payload,) = out
                elif edge:
                    acc, col = out
                    rim_col = rim_col + col
                else:
                    acc, col = out
                    col_parts[c] = col_parts[c] + col

    got = lax.all_to_all(payload, ("grp", "row"), split_axis=0, concat_axis=0, tiled=True)
    depth = INNER // members
    lines = hyper * outer // LANES
    row_sum = jnp.sum(got[:, : lines * depth], axis=0).reshape(lines, depth, hyper // lines, outer)
    row_traces = row_sum.transpose(0, 2, 1, 3).reshape(hyper, depth * outer)
    col_all = jnp.sum(got[:, lines * depth :, :block].reshape(groups, shards, 2, hyper, block), axis=0)
    col_all = col_all.transpose(1, 2, 0, 3).reshape(2, hyper, half_len)
    col_traces = jnp.concatenate([col_all[0], col_all[1, :, :1], col_all[1, :, :0:-1]], axis=1)
    return (row_traces, col_traces)


def solution(mesh):
    placed = (P("grp", "row", None), P("grp", "row", None), P(), P())
    return jax.shard_map(
        local, mesh=mesh, in_specs=placed, out_specs=(P(None, ("grp", "row")), P()), check_vma=False
    )
```

```python
import functools
import math

import jax
import jax.numpy as jnp
import numpy as np
from jax import lax
from jax.experimental import pallas as pl
from jax.experimental.pallas import tpu as pltpu
from jax.sharding import PartitionSpec as P

LANES = 128
COLS = 64
INNER = 128
FINE = 64
TILE = 16
GROUP = 8
VMEM_LIMIT = 60 * 1024 * 1024


matmul = functools.partial(jnp.dot, preferred_element_type=jnp.float32)


def split(x):
    high = x.astype(jnp.bfloat16)
    return high, (x - high.astype(jnp.float32)).astype(jnp.bfloat16)


def split_plain(x):
    high = lax.reduce_precision(x, 8, 7)
    return high.astype(jnp.bfloat16), (x - high).astype(jnp.bfloat16)


def column_tables(second_len, shards, chunks):
    half = second_len // 2
    j = (
        np.arange(shards)[None, :, None] * (half // shards)
        + np.arange(chunks)[:, None, None] * COLS
        + np.arange(COLS)
    )
    freq = np.stack([j, np.where(j == 0, half, j)], axis=2).reshape(chunks, 1, -1)
    turn = np.stack([np.zeros(j.shape), np.where(j == 0, 0.0, 0.5 * math.pi)], axis=2).reshape(chunks, 1, -1)
    unit = 2.0 * math.pi / second_len
    coarse = np.arange(second_len // FINE)[None, :, None] * FINE
    big = (coarse * freq % second_len) * unit + turn
    small = (np.arange(FINE)[None, :, None] * freq % second_len) * unit
    return [t.astype(np.float32) for t in (np.cos(big), np.sin(big), np.cos(small), np.sin(small))]


def pieces_of(chunk):
    return (48, INNER - 48) if chunk == 0 else (INNER - 32, 32)


def inner_table(spans):
    k = np.arange(INNER)
    phase = (k[:, None] * k[None, :] % INNER) * (2.0 * math.pi / INNER)
    cos, sin = np.cos(phase), np.sin(phase)
    parts, at = [], 0
    for span in spans:
        c, s = cos[:, at : at + span], sin[:, at : at + span]
        parts += [np.concatenate([c, -s]), np.concatenate([s, c])]
        at += span
    table = np.concatenate(parts, axis=1).astype(np.float32)
    high = table.astype(jnp.bfloat16)
    return high, (table - high.astype(np.float32)).astype(jnp.bfloat16)


def rotate(x, count, size, sign):
    re, im = x
    count = (count * sign) % size
    if count == 0:
        return re, im
    if 4 * count == size:
        return -im, re
    if 2 * count == size:
        return -re, -im
    if 4 * count == 3 * size:
        return im, -re
    cos, sin = math.cos(2 * math.pi * count / size), math.sin(2 * math.pi * count / size)
    if (8 * count) % size == 0:
        c, s = (1 if cos > 0 else -1), (1 if sin > 0 else -1)
        root = math.sqrt(0.5)
        return (c * root) * (re - im if c == s else re + im), (s * root) * (re + im if c == s else re - im)
    return re * cos - im * sin, re * sin + im * cos


def small_fft(xs, sign):
    n = len(xs)
    if n == 1:
        return xs
    even, odd = small_fft(xs[0::2], sign), small_fft(xs[1::2], sign)
    first, second = [], []
    for k in range(n // 2):
        (er, ei), (tr, ti) = even[k], rotate(odd[k], k, n, sign)
        first.append((er + tr, ei + ti))
        second.append((er - tr, ei - ti))
    return first + second


def columns_kernel(shards, ahead, pos_ref, p_ref, s_ref, cb_ref, sb_ref, cs_ref, ss_ref, *refs):
    outs, (high_ref, low_ref) = refs[:-2], refs[-2:]

    @pl.when(pl.program_id(0) == 0)
    def _():
        for m, distance in enumerate(ahead):
            target = lax.rem(pos_ref[0] + distance, shards)
            lanes = pl.ds(pl.multiple_of(target * LANES, LANES), LANES)
            cos, sin = cs_ref[:, lanes], ss_ref[:, lanes]

            @pl.loop(0, cb_ref.shape[0], unroll=4)
            def _(b, m=m, lanes=lanes, cos=cos, sin=sin):
                rows = pl.ds(pl.multiple_of(b * FINE, FINE), FINE)
                high, low = split(cb_ref[b, :, lanes] * cos - sb_ref[b, :, lanes] * sin)
                high_ref[rows, m * LANES : (m + 1) * LANES] = high
                low_ref[rows, m * LANES : (m + 1) * LANES] = low

    shape = outs[0].shape[1:]
    rows = shape[0] * shape[1]
    p = p_ref[...].reshape(rows, p_ref.shape[2])
    s = s_ref[...].reshape(rows, s_ref.shape[2])
    lower = lax.broadcasted_iota(jnp.int32, (rows, LANES), 1) < COLS
    wide = 2 * LANES
    for pair in range(len(ahead) // 2):
        at = slice(pair * wide, (pair + 1) * wide)
        first = matmul(p, high_ref[:, at]) + matmul(p, low_ref[:, at])
        second = matmul(s, high_ref[:, at]) + matmul(s, low_ref[:, at])
        for m in range(2):
            a, b = first[:, m * LANES : (m + 1) * LANES], second[:, m * LANES : (m + 1) * LANES]
            out = outs[2 * pair + m]
            out[0] = jnp.where(lower, a, pltpu.roll(b, COLS, 1)).reshape(shape)
            out[1] = jnp.where(lower, pltpu.roll(a, COLS, 1), b).reshape(shape)


def columns(p, s, tables, position, shards, ahead, begin, span):
    rows, second_len = p.shape
    depth = rows // INNER
    per_step = max(1, depth // 2)
    lanes = len(ahead) * LANES
    tables = [t[:, None] if n < 2 else t for n, t in enumerate(tables)]
    p, s = (x.reshape(depth, INNER, second_len) for x in (p, s))
    whole = lambda a: pl.BlockSpec(a.shape, lambda i, pos: (0,) * a.ndim)
    return pl.pallas_call(
        functools.partial(columns_kernel, shards, ahead),
        grid_spec=pltpu.PrefetchScalarGridSpec(
            num_scalar_prefetch=1,
            grid=(depth // per_step,),
            in_specs=[
                pl.BlockSpec(
                    (pl.Element(per_step), pl.Element(span), pl.Element(second_len)),
                    lambda i, pos: (i * per_step, begin, 0),
                )
            ]
            * 2
            + [whole(t) for t in tables],
            out_specs=[pl.BlockSpec((2, per_step, span, LANES), lambda i, pos: (0, i, 0, 0))] * len(ahead),
            scratch_shapes=[pltpu.VMEM((second_len, len(ahead) * LANES), jnp.bfloat16)] * 2,
        ),
        out_shape=[jax.ShapeDtypeStruct((2, depth, span, LANES), jnp.float32)] * len(ahead),
        compiler_params=pltpu.CompilerParams(vmem_limit_bytes=VMEM_LIMIT),
        cost_estimate=pl.CostEstimate(
            flops=8 * depth * span * second_len * lanes,
            bytes_accessed=4 * depth * span * second_len + 8 * lanes * depth * span,
            transcendentals=0,
        ),
        name="columns",
    )(position, p, s, *tables)


def outer_tile(edge, inputs, rows, turns, tmp_ref, store):
    shards, depth = len(inputs), inputs[0].shape[1]
    outer = shards * depth
    lane = lax.broadcasted_iota(jnp.int32, (TILE, LANES), 1) % COLS
    for g in range(depth):
        xs = []
        for ref in inputs:
            re, im = ref[0, g, rows], ref[1, g, rows]
            if edge:
                re = jnp.where(lane == 0, re, jnp.where(lane == 1, pltpu.roll(im, 1, 1), 0.0))
                im = jnp.zeros_like(re)
            xs.append((re, im))
        for q, y in enumerate(small_fft(xs, 1)):
            tmp_ref[q, 0, g], tmp_ref[q, 1, g] = rotate(y, g * q, outer, -1)
    for q in range(shards):
        zs = small_fft([(tmp_ref[q, 0, g], tmp_ref[q, 1, g]) for g in range(depth)], -1)
        for r, (re, im) in enumerate(zs):
            k = q + shards * r
            cos = jnp.broadcast_to(turns[:, k : k + 1], (TILE, LANES))
            sin = jnp.broadcast_to(turns[:, outer + k : outer + k + 1], (TILE, LANES))
            store(k, 0, *split(re * cos - im * sin))
            store(k, 1, *split(re * sin + im * cos))


def outer_kernel(edge, begin, *refs):
    turn_ref, high_ref, low_ref, tmp_ref = refs[-4:]
    inputs = refs[:-4]
    span = inputs[0].shape[2]

    @pl.loop(0, span // TILE)
    def _(t):
        rows = pl.ds(pl.multiple_of(t * TILE, TILE), TILE)

        def store(k, plane, high, low):
            high_ref[k, plane, rows, :] = high
            low_ref[k, plane, rows, :] = low

        first = pl.multiple_of(begin + pl.program_id(0) * span + t * TILE, TILE)
        outer_tile(edge, inputs, rows, turn_ref[pl.ds(first, TILE), :], tmp_ref, store)


def outer_stage(pieces, turns, begin, edge):
    shards = len(pieces)
    _, depth, span, _ = pieces[0].shape
    outer = shards * depth
    steps = next(n for n in (3, 2, 1) if span % (n * TILE) == 0)
    rows = span // steps
    return pl.pallas_call(
        functools.partial(outer_kernel, edge, begin),
        grid=(steps,),
        in_specs=[pl.BlockSpec((2, depth, rows, LANES), lambda i: (0, 0, i, 0))] * shards
        + [pl.BlockSpec(turns.shape, lambda i: (0, 0))],
        out_specs=[pl.BlockSpec((outer, 2, rows, LANES), lambda i: (0, 0, i, 0))] * 2,
        out_shape=[jax.ShapeDtypeStruct((outer, 2, span, LANES), jnp.bfloat16)] * 2,
        scratch_shapes=[pltpu.VMEM((shards, 2, depth, TILE, LANES), jnp.float32)],
        compiler_params=pltpu.CompilerParams(vmem_limit_bytes=VMEM_LIMIT),
        cost_estimate=pl.CostEstimate(
            flops=200 * outer * span * LANES, bytes_accessed=16 * outer * span * LANES, transcendentals=0
        ),
        name="outer",
    )(*pieces, turns)


def early_kernel(shards, begin, *refs):
    inputs, (turn_ref, table_ref, sums_ref, e_ref, tmp_ref) = refs[:shards], refs[shards:]
    span = inputs[0].shape[2]
    three_outer(False, inputs, begin, turn_ref, tmp_ref, e_ref)

    @pl.loop(0, sums_ref.shape[0])
    def _(step):
        e = jnp.concatenate([e_ref[GROUP * step + n] for n in range(GROUP)], axis=1)
        sums_ref[step] = matmul(table_ref[...], e)


def three_outer(edge, inputs, begin, turn_ref, tmp_ref, e_ref):
    span = inputs[0].shape[2]

    @pl.loop(0, span // TILE)
    def _(t):
        rows = pl.ds(pl.multiple_of(t * TILE, TILE), TILE)

        def store(k, plane, high, low):
            for term, value in enumerate((high, low, high)):
                at = pl.ds(pl.multiple_of((2 * term + plane) * span + t * TILE, TILE), TILE)
                e_ref[k, at, :] = value

        first = pl.multiple_of(begin + t * TILE, TILE)
        outer_tile(edge, inputs, rows, turn_ref[pl.ds(first, TILE), :], tmp_ref, store)


def three_table(table, begin, span):
    high, low = (t[:, 2 * begin : 2 * (begin + span)] for t in table)
    return np.concatenate([high, high, low], axis=1)


def early_stage(pieces, turns, begin, table):
    shards = len(pieces)
    _, depth, span, _ = pieces[0].shape
    outer = shards * depth
    table = three_table(table, begin, span)
    whole = lambda a: pl.BlockSpec(a.shape, lambda i: (0,) * len(a.shape))
    out = jax.ShapeDtypeStruct((outer // GROUP, 2 * INNER, GROUP * LANES), jnp.float32)
    return pl.pallas_call(
        functools.partial(early_kernel, shards, begin),
        grid=(1,),
        in_specs=[whole(a) for a in (*pieces, turns, table)],
        out_specs=whole(out),
        out_shape=out,
        scratch_shapes=[
            pltpu.VMEM((outer, 6 * span, LANES), jnp.bfloat16),
            pltpu.VMEM((shards, 2, depth, TILE, LANES), jnp.float32),
        ],
        compiler_params=pltpu.CompilerParams(vmem_limit_bytes=VMEM_LIMIT),
        cost_estimate=pl.CostEstimate(
            flops=2 * 3 * 4 * outer * INNER * span * LANES,
            bytes_accessed=8 * outer * (span + INNER) * LANES,
            transcendentals=0,
        ),
        name="early",
    )(*pieces, turns, table)


def inner_kernel(shards, begin, edge, members, *refs):
    last = members > 0
    inputs, refs = refs[:shards], refs[shards:]
    if last:
        turn_ref, table_ref, cw_ref, sums_hbm, rr_hbm, in_ref = refs[:6]
        refs = refs[6:]
    else:
        turn_ref, th_ref, tl_ref, cw_ref, prev_high, prev_low, rr_hbm, in_ref = refs[:8]
        refs = refs[8:]
    late = []
    if last:
        ahead_hbm, behind_hbm, before_ref, keep_ref, pay_ref, acc_ref, fin_ref, ahead_ref, behind_ref = refs[:9]
        refs = refs[9:]
        late = [(ahead_hbm, ahead_ref), (behind_hbm, behind_ref)]
    else:
        acc_ref, col_ref = refs[:2]
        refs = refs[2:]
    if last:
        e_ref, sums_ref, tmp_ref, sum_ref, rr_ref, sems = refs
        arrived = [(sums_hbm, sums_ref)]
    else:
        high_ref, low_ref, tmp_ref, sum_ref, rr_ref, sems = refs
        early = prev_high.shape[1]
        rows = pl.ds(0, early)
        arrived = [(prev_high, high_ref.at[:, rows, :]), (prev_low, low_ref.at[:, rows, :])]
    hypers = cw_ref.shape[1] // (2 * GROUP)
    first = len(arrived) + 2
    copies = [
        pltpu.make_async_copy(source, target, sems.at[n])
        for n, (source, target) in enumerate(
            arrived + [(rr_hbm, rr_ref), (in_ref, acc_ref)] + late
        )
    ]
    for copy in copies:
        copy.start()
    span = inputs[0].shape[2]
    if last:
        three_outer(edge, inputs, begin, turn_ref, tmp_ref, e_ref)
    else:
        @pl.loop(0, span // TILE)
        def _(t):
            rows = pl.ds(pl.multiple_of(t * TILE, TILE), TILE)

            def store(k, plane, high, low):
                at = pl.ds(pl.multiple_of(early + plane * span + t * TILE, TILE), TILE)
                high_ref[k, at, :] = high
                low_ref[k, at, :] = low

            first = pl.multiple_of(begin + t * TILE, TILE)
            outer_tile(edge, inputs, rows, turn_ref[pl.ds(first, TILE), :], tmp_ref, store)

    for copy in copies[:first]:
        copy.wait()
    lower = lax.broadcasted_iota(jnp.int32, (INNER, LANES), 1) < COLS
    sum_ref[...] = jnp.zeros_like(sum_ref)

    @pl.loop(0, acc_ref.shape[0])
    def _(step):
        total = acc_ref[step]
        part = 0.0
        for block in range(GROUP // 8):
            ks = [GROUP * step + 8 * block + n for n in range(8)]
            if last:
                out = sums_ref[step] + matmul(table_ref[...], jnp.concatenate([e_ref[k] for k in ks], axis=1))
            else:
                table = jnp.concatenate([th_ref[...], th_ref[...], tl_ref[...]], axis=1)
                high = jnp.concatenate([high_ref[k] for k in ks], axis=1)
                low = jnp.concatenate([low_ref[k] for k in ks], axis=1)
                out = matmul(table, jnp.concatenate([high, low, high], axis=0))
            xs = []
            for pair in range(8 // 2):
                x = 0.0
                for plane in range(2):
                    z = out[plane * INNER : (plane + 1) * INNER, 2 * pair * LANES : 2 * (pair + 1) * LANES]
                    a, b = z[:, :LANES], z[:, LANES:]
                    x += jnp.where(lower, a, b) * pltpu.roll(jnp.where(lower, b, a), COLS, 1)
                xs.append(jnp.concatenate(split(x), axis=1))
            x = jnp.concatenate(xs, axis=0)
            r = matmul(x, cw_ref[...])
            r = r[:, :LANES] + r[:, LANES:]
            for pair in range(8 // 2):
                turn = 2 * hypers * (8 // 2 * block + pair)
                one = r[pair * INNER : (pair + 1) * INNER]
                total += pltpu.roll(one, turn, 1) if turn else one
            for quad in range(8 // 4):
                part += matmul(
                    rr_ref[GROUP // 4 * step + 8 // 4 * block + quad],
                    x[2 * quad * INNER : 2 * (quad + 1) * INNER],
                )
        sum_ref[...] += part
        acc_ref[step] = total

    t = sum_ref[...]
    both = []
    for n in range(2):
        at = 2 * n * hypers
        both.append(
            t[at : at + hypers, :LANES] + t[at + hypers : at + 2 * hypers, :LANES] + t[at : at + hypers, LANES:]
        )
    col = both[0] + pltpu.roll(both[1], COLS, 1)
    if not last:
        col_ref[...] = col
        return

    for copy in copies[first:]:
        copy.wait()
    outer = fin_ref.shape[1] * 2 // hypers
    acc = jnp.concatenate([acc_ref[n] for n in range(acc_ref.shape[0])], axis=1)
    parts = split(acc)
    ahead = sum(matmul(part, ahead_ref[...]) for part in parts)
    behind = sum(matmul(part, behind_ref[...]) for part in parts)
    column = lax.broadcasted_iota(jnp.int32, behind.shape, 1)
    behind = jnp.where(column % outer == 0, pltpu.roll(behind, INNER - 1, 0), behind)
    row = lax.broadcasted_iota(jnp.int32, (INNER, INNER), 0)
    column = lax.broadcasted_iota(jnp.int32, (INNER, INNER), 1)
    flip = jnp.where(row + column == INNER - 1, 1.0, 0.0).astype(jnp.bfloat16)
    fin_ref[...] = ahead + sum(matmul(flip, part) for part in split(behind))

    mine = before_ref[...] + keep_ref[0] * col + keep_ref[1] * pltpu.roll(col, COLS, 1)
    depth = INNER // members
    groups = fin_ref.shape[1] // LANES
    for d in range(members):
        for n in range(groups):
            pay_ref[d, n * depth : (n + 1) * depth, :] = fin_ref[
                d * depth : (d + 1) * depth, n * LANES : (n + 1) * LANES
            ]
        pay_ref[d, groups * depth :, :] = mine


def inner_stage(pieces, turns, begin, edge, early, table, rr, cw, acc, closing):
    shards = len(pieces)
    _, depth, span, _ = pieces[0].shape
    outer = shards * depth
    hypers = 2 * LANES // (2 * GROUP)
    whole = lambda a: pl.BlockSpec(a.shape, lambda i: (0,) * len(a.shape))
    scratch = []
    members = 0
    if closing:
        orders, before, keep, members = closing
        extra, small = list(orders), [before, keep]
        table = [three_table(table, begin, span)]
        early = [early]
        held = [pltpu.VMEM((outer, 6 * span, LANES), jnp.bfloat16), pltpu.VMEM(early[0].shape, jnp.float32)]
        lines = hypers // 2 * outer // LANES * (INNER // members) + hypers
        out_shape = [jax.ShapeDtypeStruct((members, lines, LANES), jnp.float32)]
        scratch = [
            pltpu.VMEM(acc.shape, jnp.float32),
            pltpu.VMEM((INNER, hypers // 2 * outer), jnp.float32),
            *[pltpu.VMEM(o.shape, o.dtype) for o in orders],
        ]
    else:
        extra, small = [], []
        early = [f.reshape(outer, -1, LANES) for f in early]
        held = [pltpu.VMEM((outer, 2 * INNER, LANES), jnp.bfloat16)] * 2
        out_shape = [
            jax.ShapeDtypeStruct(acc.shape, jnp.float32),
            jax.ShapeDtypeStruct((hypers, LANES), jnp.float32),
        ]
    return pl.pallas_call(
        functools.partial(inner_kernel, shards, begin, edge, members),
        grid=(1,),
        in_specs=[whole(a) for a in (*pieces, turns, *table, cw)]
        + [pl.BlockSpec(memory_space=pl.ANY)] * (len(early) + 2 + len(extra))
        + [whole(a) for a in small],
        out_specs=[whole(a) for a in out_shape],
        out_shape=out_shape,
        scratch_shapes=scratch
        + [
            *held,
            pltpu.VMEM((shards, 2, depth, TILE, LANES), jnp.float32),
            pltpu.VMEM((4 * hypers, 2 * LANES), jnp.float32),
            pltpu.VMEM(rr.shape, rr.dtype),
            pltpu.SemaphoreType.DMA((len(early) + 2 + len(extra),)),
        ],
        compiler_params=pltpu.CompilerParams(vmem_limit_bytes=VMEM_LIMIT),
        cost_estimate=pl.CostEstimate(
            flops=2 * 3 * 4 * outer * INNER * INNER * LANES,
            bytes_accessed=8 * outer * INNER * LANES,
            transcendentals=0,
        ),
        name="inner",
    )(*pieces, turns, *table, cw, *early, rr, acc, *extra, *small)


def orders_kernel(ahead_ref, behind_ref):
    lanes, width = ahead_ref.shape
    hypers = LANES // GROUP
    outer = lanes // hypers
    row = lax.broadcasted_iota(jnp.int32, (lanes, width), 0)
    column = lax.broadcasted_iota(jnp.int32, (lanes, width), 1)
    k, h = column % outer, column // outer
    one = lambda hit: jnp.where(hit, 1.0, 0.0).astype(jnp.bfloat16)
    ahead_ref[...] = one(row == hypers * k + h)
    behind_ref[...] = one(row == hypers * ((outer - k) % outer) + hypers // 2 + h)


def output_orders(outer, hyper):
    shape = jax.ShapeDtypeStruct((2 * hyper * outer, hyper * outer), jnp.bfloat16)
    return pl.pallas_call(
        orders_kernel,
        out_shape=[shape, shape],
        compiler_params=pltpu.CompilerParams(vmem_limit_bytes=VMEM_LIMIT),
        cost_estimate=pl.CostEstimate(flops=0, bytes_accessed=4 * shape.size, transcendentals=0),
        name="orders",
    )()


def local(probes, solves, row_spectra, col_spectra):
    shards = lax.axis_size("row")
    groups = lax.axis_size("grp")
    position = lax.axis_index("row")
    local_probes, rows, second_len = probes.shape
    hyper, first_len = row_spectra.shape
    half_len = second_len // 2
    block = half_len // shards
    chunks = block // COLS
    outer = first_len // INNER
    scale = 1.0 / (local_probes * groups * first_len * second_len)

    tables = column_tables(second_len, shards, chunks)
    where_am_i = position.astype(jnp.int32).reshape(1)

    k = jnp.arange(outer, dtype=jnp.int32)
    count = k[:, None] * jnp.arange(INNER, dtype=jnp.int32)[None, :] + (k % shards * position * rows)[:, None]
    phase = (count % first_len).astype(jnp.float32) * (2.0 * math.pi / first_len)
    turns = jnp.concatenate([jnp.cos(phase), -jnp.sin(phase)], axis=0).T

    forward = row_spectra.reshape(hyper, INNER, outer).transpose(0, 2, 1) * scale
    i = np.arange(INNER)
    exact = functools.partial(jnp.einsum, precision=lax.Precision.HIGHEST)
    turned = exact("mn,hnk->hmk", np.eye(outer, dtype=np.float32)[-np.arange(outer) % outer], forward)
    mirror = jnp.concatenate(
        [
            exact("hmk,ka->hma", turned[:, :1], np.eye(INNER, dtype=np.float32)[-i % INNER]),
            exact("hmk,ka->hma", turned[:, 1:], np.eye(INNER, dtype=np.float32)[INNER - 1 - i]),
        ],
        axis=1,
    )
    rr = jnp.concatenate([forward, mirror], axis=0)
    rr = rr.reshape(2 * hyper, outer // 4, 2, 2, INNER).transpose(1, 3, 0, 2, 4)
    rr = jnp.stack(split_plain(rr), axis=2).reshape(outer // 4, 8 * hyper, 2 * INNER)

    start = position * block
    ahead = lax.dynamic_slice_in_dim(col_spectra, start, block, 1)
    reverse = jnp.concatenate(
        [col_spectra[:, half_len : half_len + 1], col_spectra[:, :half_len:-1]], axis=1
    )
    behind = lax.dynamic_slice_in_dim(reverse, start, block, 1)
    edge_column = jnp.logical_and(position == 0, jnp.arange(block) == 0)
    both = jnp.concatenate([ahead, behind], axis=0) * scale
    main = jnp.where(edge_column, 0.0, both).reshape(2 * hyper, chunks, COLS).transpose(1, 2, 0)
    rim = jnp.where(position == 0, both[:, 0].reshape(2, hyper), 0.0)
    rim = jnp.pad(rim, ((0, COLS - 2), (0, hyper)))
    cw = jnp.concatenate([main, rim[None]], axis=0)
    cw = jnp.concatenate(
        [
            jnp.pad(cw, ((0, 0), (0, 0), (0, LANES - 2 * hyper))),
            jnp.pad(cw, ((0, 0), (0, 0), (2 * hyper, LANES - 4 * hyper))),
        ],
        axis=1,
    )
    high, low = split_plain(cw)
    cw = jnp.concatenate(
        [jnp.concatenate([high, low], axis=2), jnp.concatenate([high, jnp.zeros_like(low)], axis=2)], axis=1
    )
    orders = output_orders(outer, hyper)

    members = groups * shards
    order = [shards // 2, shards // 4, 3 * shards // 4, 3]
    order += [m for m in range(1, shards) if m not in order] + [0]
    moved = []

    def send(n, c, begin, span, after=None):
        fields = probes[n], solves[n]
        if after is not None:
            *fields, _ = lax.optimization_barrier((*fields, after))
        sent = {}
        for ahead in (order,) if moved else (order[:2], order[2:4], order[4:]):
            out = columns(*fields, [t[c] for t in tables], where_am_i, shards, ahead, begin, span)
            sent.update(zip(ahead, out))
        for m in order[:-1]:
            sent[m] = lax.ppermute(sent[m], "row", [(i, (i + m) % shards) for i in range(shards)])
        moved.append([sent[m] for m in range(shards)])

    todo = [
        (n, c, sum(pieces_of(c)[:at]), span)
        for n in range(local_probes)
        for c in range(chunks)
        for at, span in enumerate(pieces_of(c))
    ]
    early_sends = todo if len(todo) < 4 else todo[:-1]
    for piece in early_sends:
        send(*piece)
    acc = jnp.zeros((outer // GROUP, INNER, LANES), jnp.float32)
    col_parts = [0.0] * chunks
    rim_col = 0.0
    slots = np.arange(LANES)
    for n in range(local_probes):
        for c in range(chunks):
            spans = pieces_of(c)
            table = inner_table(spans)
            at = 2 * (n * chunks + c)
            if at + 2 > len(moved):
                send(*todo[-1], after=col)
            first, second = moved[at : at + 2]
            for edge in (True, False) if c == 0 else (False,):
                closing = None
                if not (n == local_probes - 1 and c == chunks - 1 and not edge):
                    early = outer_stage(first, turns, 0, edge)
                else:
                    early = early_stage(first, turns, 0, table)
                    rim_first = jnp.concatenate([rim_col[:hyper, 0], rim_col[:hyper, 1]])[:, None]
                    rim_first = jnp.where(jnp.logical_and(position == 0, slots == 0), rim_first, 0.0)
                    clear = jnp.where(jnp.logical_and(position == 0, slots == 0), 0.0, 1.0)
                    mine = jnp.pad(
                        jnp.concatenate(
                            [jnp.zeros((2 * hyper, 0), jnp.float32)]
                            + [
                                jnp.broadcast_to(part, (2 * hyper, LANES))[:, :COLS] + jnp.zeros((2 * hyper, COLS))
                                for part in col_parts
                            ],
                            axis=1,
                        ),
                        ((0, 0), (0, LANES - chunks * COLS)),
                    )
                    before = mine * clear + rim_first
                    keep = jnp.stack(
                        [jnp.where((slots // COLS == c) & (c == k), clear, 0.0) for k in range(2)]
                    )
                    keep = jnp.broadcast_to(keep[:, None], (2, 2 * hyper, LANES))
                    closing = (orders, before, keep, members)
                out = inner_stage(
                    second, turns, spans[0], edge, early, table, rr, cw[chunks if edge else c], acc, closing
                )
                if closing:
                    (payload,) = out
                elif edge:
                    acc, col = out
                    rim_col = rim_col + col
                else:
                    acc, col = out
                    col_parts[c] = col_parts[c] + col

    got = lax.all_to_all(payload, ("grp", "row"), split_axis=0, concat_axis=0, tiled=True)
    depth = INNER // members
    lines = hyper * outer // LANES
    row_sum = jnp.sum(got[:, : lines * depth], axis=0).reshape(lines, depth, hyper // lines, outer)
    row_traces = row_sum.transpose(0, 2, 1, 3).reshape(hyper, depth * outer)
    col_all = jnp.sum(got[:, lines * depth :, :block].reshape(groups, shards, 2, hyper, block), axis=0)
    col_all = col_all.transpose(1, 2, 0, 3).reshape(2, hyper, half_len)
    col_traces = jnp.concatenate([col_all[0], col_all[1, :, :1], col_all[1, :, :0:-1]], axis=1)
    return (row_traces, col_traces)


def solution(mesh):
    placed = (P("grp", "row", None), P("grp", "row", None), P(), P())
    return jax.shard_map(
        local, mesh=mesh, in_specs=placed, out_specs=(P(None, ("grp", "row")), P()), check_vma=False
    )
```

```python
import functools
import math

import jax
import jax.numpy as jnp
import numpy as np
from jax import lax
from jax.experimental import pallas as pl
from jax.experimental.pallas import tpu as pltpu
from jax.sharding import PartitionSpec as P

LANES = 128
COLS = 64
INNER = 128
FINE = 64
TILE = 16
GROUP = 8
VMEM_LIMIT = 60 * 1024 * 1024


matmul = functools.partial(jnp.dot, preferred_element_type=jnp.float32)


def split(x):
    high = x.astype(jnp.bfloat16)
    return high, (x - high.astype(jnp.float32)).astype(jnp.bfloat16)


def split_plain(x):
    high = lax.reduce_precision(x, 8, 7)
    return high.astype(jnp.bfloat16), (x - high).astype(jnp.bfloat16)


def column_tables(second_len, shards, chunks):
    half = second_len // 2
    j = (
        np.arange(shards)[None, :, None] * (half // shards)
        + np.arange(chunks)[:, None, None] * COLS
        + np.arange(COLS)
    )
    freq = np.stack([j, np.where(j == 0, half, j)], axis=2).reshape(chunks, 1, -1)
    turn = np.stack([np.zeros(j.shape), np.where(j == 0, 0.0, 0.5 * math.pi)], axis=2).reshape(chunks, 1, -1)
    unit = 2.0 * math.pi / second_len
    coarse = np.arange(second_len // FINE)[None, :, None] * FINE
    big = (coarse * freq % second_len) * unit + turn
    small = (np.arange(FINE)[None, :, None] * freq % second_len) * unit
    return [t.astype(np.float32) for t in (np.cos(big), np.sin(big), np.cos(small), np.sin(small))]


def pieces_of(chunk):
    return (48, INNER - 48) if chunk == 0 else (INNER - 32, 32)


def inner_table(spans):
    k = np.arange(INNER)
    phase = (k[:, None] * k[None, :] % INNER) * (2.0 * math.pi / INNER)
    cos, sin = np.cos(phase), np.sin(phase)
    parts, at = [], 0
    for span in spans:
        c, s = cos[:, at : at + span], sin[:, at : at + span]
        parts += [np.concatenate([c, -s]), np.concatenate([s, c])]
        at += span
    table = np.concatenate(parts, axis=1).astype(np.float32)
    high = table.astype(jnp.bfloat16)
    return high, (table - high.astype(np.float32)).astype(jnp.bfloat16)


def rotate(x, count, size, sign):
    re, im = x
    count = (count * sign) % size
    if count == 0:
        return re, im
    if 4 * count == size:
        return -im, re
    if 2 * count == size:
        return -re, -im
    if 4 * count == 3 * size:
        return im, -re
    cos, sin = math.cos(2 * math.pi * count / size), math.sin(2 * math.pi * count / size)
    if (8 * count) % size == 0:
        c, s = (1 if cos > 0 else -1), (1 if sin > 0 else -1)
        root = math.sqrt(0.5)
        return (c * root) * (re - im if c == s else re + im), (s * root) * (re + im if c == s else re - im)
    return re * cos - im * sin, re * sin + im * cos


def small_fft(xs, sign):
    n = len(xs)
    if n == 1:
        return xs
    even, odd = small_fft(xs[0::2], sign), small_fft(xs[1::2], sign)
    first, second = [], []
    for k in range(n // 2):
        (er, ei), (tr, ti) = even[k], rotate(odd[k], k, n, sign)
        first.append((er + tr, ei + ti))
        second.append((er - tr, ei - ti))
    return first + second


def columns_kernel(shards, ahead, pos_ref, p_ref, s_ref, cb_ref, sb_ref, cs_ref, ss_ref, *refs):
    outs, (high_ref, low_ref) = refs[:-2], refs[-2:]

    @pl.when(pl.program_id(0) == 0)
    def _():
        for m, distance in enumerate(ahead):
            target = lax.rem(pos_ref[0] + distance, shards)
            lanes = pl.ds(pl.multiple_of(target * LANES, LANES), LANES)
            cos, sin = cs_ref[:, lanes], ss_ref[:, lanes]

            @pl.loop(0, cb_ref.shape[0], unroll=4)
            def _(b, m=m, lanes=lanes, cos=cos, sin=sin):
                rows = pl.ds(pl.multiple_of(b * FINE, FINE), FINE)
                high, low = split(cb_ref[b, :, lanes] * cos - sb_ref[b, :, lanes] * sin)
                high_ref[rows, m * LANES : (m + 1) * LANES] = high
                low_ref[rows, m * LANES : (m + 1) * LANES] = low

    shape = outs[0].shape[1:]
    rows = shape[0] * shape[1]
    p = p_ref[...].reshape(rows, p_ref.shape[2])
    s = s_ref[...].reshape(rows, s_ref.shape[2])
    lower = lax.broadcasted_iota(jnp.int32, (rows, LANES), 1) < COLS
    wide = 2 * LANES
    for pair in range(len(ahead) // 2):
        at = slice(pair * wide, (pair + 1) * wide)
        first = matmul(p, high_ref[:, at]) + matmul(p, low_ref[:, at])
        second = matmul(s, high_ref[:, at]) + matmul(s, low_ref[:, at])
        for m in range(2):
            a, b = first[:, m * LANES : (m + 1) * LANES], second[:, m * LANES : (m + 1) * LANES]
            out = outs[2 * pair + m]
            out[0] = jnp.where(lower, a, pltpu.roll(b, COLS, 1)).reshape(shape)
            out[1] = jnp.where(lower, pltpu.roll(a, COLS, 1), b).reshape(shape)


def columns(p, s, tables, position, shards, ahead, begin, span):
    rows, second_len = p.shape
    depth = rows // INNER
    per_step = max(1, depth // 2)
    lanes = len(ahead) * LANES
    tables = [t[:, None] if n < 2 else t for n, t in enumerate(tables)]
    p, s = (x.reshape(depth, INNER, second_len) for x in (p, s))
    whole = lambda a: pl.BlockSpec(a.shape, lambda i, pos: (0,) * a.ndim)
    return pl.pallas_call(
        functools.partial(columns_kernel, shards, ahead),
        grid_spec=pltpu.PrefetchScalarGridSpec(
            num_scalar_prefetch=1,
            grid=(depth // per_step,),
            in_specs=[
                pl.BlockSpec(
                    (pl.Element(per_step), pl.Element(span), pl.Element(second_len)),
                    lambda i, pos: (i * per_step, begin, 0),
                )
            ]
            * 2
            + [whole(t) for t in tables],
            out_specs=[pl.BlockSpec((2, per_step, span, LANES), lambda i, pos: (0, i, 0, 0))] * len(ahead),
            scratch_shapes=[pltpu.VMEM((second_len, len(ahead) * LANES), jnp.bfloat16)] * 2,
        ),
        out_shape=[jax.ShapeDtypeStruct((2, depth, span, LANES), jnp.float32)] * len(ahead),
        compiler_params=pltpu.CompilerParams(vmem_limit_bytes=VMEM_LIMIT),
        cost_estimate=pl.CostEstimate(
            flops=8 * depth * span * second_len * lanes,
            bytes_accessed=4 * depth * span * second_len + 8 * lanes * depth * span,
            transcendentals=0,
        ),
        name="columns",
    )(position, p, s, *tables)


def outer_tile(edge, inputs, rows, turns, tmp_ref, store):
    shards, depth = len(inputs), inputs[0].shape[1]
    outer = shards * depth
    lane = lax.broadcasted_iota(jnp.int32, (TILE, LANES), 1) % COLS
    for g in range(depth):
        xs = []
        for ref in inputs:
            re, im = ref[0, g, rows], ref[1, g, rows]
            if edge:
                re = jnp.where(lane == 0, re, jnp.where(lane == 1, pltpu.roll(im, 1, 1), 0.0))
                im = jnp.zeros_like(re)
            xs.append((re, im))
        for q, y in enumerate(small_fft(xs, 1)):
            tmp_ref[q, 0, g], tmp_ref[q, 1, g] = rotate(y, g * q, outer, -1)
    for q in range(shards):
        zs = small_fft([(tmp_ref[q, 0, g], tmp_ref[q, 1, g]) for g in range(depth)], -1)
        for r, (re, im) in enumerate(zs):
            k = q + shards * r
            cos = jnp.broadcast_to(turns[:, k : k + 1], (TILE, LANES))
            sin = jnp.broadcast_to(turns[:, outer + k : outer + k + 1], (TILE, LANES))
            store(k, 0, *split(re * cos - im * sin))
            store(k, 1, *split(re * sin + im * cos))


def outer_kernel(edge, begin, *refs):
    turn_ref, high_ref, low_ref, tmp_ref = refs[-4:]
    inputs = refs[:-4]
    span = inputs[0].shape[2]

    @pl.loop(0, span // TILE)
    def _(t):
        rows = pl.ds(pl.multiple_of(t * TILE, TILE), TILE)

        def store(k, plane, high, low):
            high_ref[k, plane, rows, :] = high
            low_ref[k, plane, rows, :] = low

        first = pl.multiple_of(begin + pl.program_id(0) * span + t * TILE, TILE)
        outer_tile(edge, inputs, rows, turn_ref[pl.ds(first, TILE), :], tmp_ref, store)


def outer_stage(pieces, turns, begin, edge):
    shards = len(pieces)
    _, depth, span, _ = pieces[0].shape
    outer = shards * depth
    steps = next(n for n in (3, 2, 1) if span % (n * TILE) == 0)
    rows = span // steps
    return pl.pallas_call(
        functools.partial(outer_kernel, edge, begin),
        grid=(steps,),
        in_specs=[pl.BlockSpec((2, depth, rows, LANES), lambda i: (0, 0, i, 0))] * shards
        + [pl.BlockSpec(turns.shape, lambda i: (0, 0))],
        out_specs=[pl.BlockSpec((outer, 2, rows, LANES), lambda i: (0, 0, i, 0))] * 2,
        out_shape=[jax.ShapeDtypeStruct((outer, 2, span, LANES), jnp.bfloat16)] * 2,
        scratch_shapes=[pltpu.VMEM((shards, 2, depth, TILE, LANES), jnp.float32)],
        compiler_params=pltpu.CompilerParams(vmem_limit_bytes=VMEM_LIMIT),
        cost_estimate=pl.CostEstimate(
            flops=200 * outer * span * LANES, bytes_accessed=16 * outer * span * LANES, transcendentals=0
        ),
        name="outer",
    )(*pieces, turns)


def early_kernel(shards, begin, *refs):
    inputs, (turn_ref, table_ref, sums_ref, e_ref, tmp_ref) = refs[:shards], refs[shards:]
    span = inputs[0].shape[2]
    three_outer(False, inputs, begin, turn_ref, tmp_ref, e_ref)

    @pl.loop(0, sums_ref.shape[0])
    def _(step):
        e = jnp.concatenate([e_ref[GROUP * step + n] for n in range(GROUP)], axis=1)
        sums_ref[step] = matmul(table_ref[...], e)


def three_outer(edge, inputs, begin, turn_ref, tmp_ref, e_ref):
    span = inputs[0].shape[2]

    @pl.loop(0, span // TILE)
    def _(t):
        rows = pl.ds(pl.multiple_of(t * TILE, TILE), TILE)

        def store(k, plane, high, low):
            for term, value in enumerate((high, low, high)):
                at = pl.ds(pl.multiple_of((2 * term + plane) * span + t * TILE, TILE), TILE)
                e_ref[k, at, :] = value

        first = pl.multiple_of(begin + t * TILE, TILE)
        outer_tile(edge, inputs, rows, turn_ref[pl.ds(first, TILE), :], tmp_ref, store)


def three_table(table, begin, span):
    high, low = (t[:, 2 * begin : 2 * (begin + span)] for t in table)
    return np.concatenate([high, high, low], axis=1)


def early_stage(pieces, turns, begin, table):
    shards = len(pieces)
    _, depth, span, _ = pieces[0].shape
    outer = shards * depth
    table = three_table(table, begin, span)
    whole = lambda a: pl.BlockSpec(a.shape, lambda i: (0,) * len(a.shape))
    out = jax.ShapeDtypeStruct((outer // GROUP, 2 * INNER, GROUP * LANES), jnp.float32)
    return pl.pallas_call(
        functools.partial(early_kernel, shards, begin),
        grid=(1,),
        in_specs=[whole(a) for a in (*pieces, turns, table)],
        out_specs=whole(out),
        out_shape=out,
        scratch_shapes=[
            pltpu.VMEM((outer, 6 * span, LANES), jnp.bfloat16),
            pltpu.VMEM((shards, 2, depth, TILE, LANES), jnp.float32),
        ],
        compiler_params=pltpu.CompilerParams(vmem_limit_bytes=VMEM_LIMIT),
        cost_estimate=pl.CostEstimate(
            flops=2 * 3 * 4 * outer * INNER * span * LANES,
            bytes_accessed=8 * outer * (span + INNER) * LANES,
            transcendentals=0,
        ),
        name="early",
    )(*pieces, turns, table)


def inner_kernel(shards, begin, edge, members, *refs):
    last = members > 0
    inputs, refs = refs[:shards], refs[shards:]
    if last:
        turn_ref, table_ref, cw_ref, sums_hbm, rr_hbm, in_ref = refs[:6]
        refs = refs[6:]
    else:
        turn_ref, th_ref, tl_ref, cw_ref, prev_high, prev_low, rr_hbm, in_ref = refs[:8]
        refs = refs[8:]
    late = []
    if last:
        ahead_hbm, behind_hbm, before_ref, keep_ref, pay_ref, acc_ref, fin_ref, ahead_ref, behind_ref = refs[:9]
        refs = refs[9:]
        late = [(ahead_hbm, ahead_ref), (behind_hbm, behind_ref)]
    else:
        acc_ref, col_ref = refs[:2]
        refs = refs[2:]
    if last:
        e_ref, sums_ref, tmp_ref, sum_ref, rr_ref, sems = refs
        arrived = [(sums_hbm, sums_ref)]
    else:
        high_ref, low_ref, tmp_ref, sum_ref, rr_ref, sems = refs
        early = prev_high.shape[1]
        rows = pl.ds(0, early)
        arrived = [(prev_high, high_ref.at[:, rows, :]), (prev_low, low_ref.at[:, rows, :])]
    hypers = cw_ref.shape[1] // (2 * GROUP)
    first = len(arrived) + 2
    copies = [
        pltpu.make_async_copy(source, target, sems.at[n])
        for n, (source, target) in enumerate(
            arrived + [(rr_hbm, rr_ref), (in_ref, acc_ref)] + late
        )
    ]
    for copy in copies:
        copy.start()
    span = inputs[0].shape[2]
    if last:
        three_outer(edge, inputs, begin, turn_ref, tmp_ref, e_ref)
    else:
        @pl.loop(0, span // TILE)
        def _(t):
            rows = pl.ds(pl.multiple_of(t * TILE, TILE), TILE)

            def store(k, plane, high, low):
                at = pl.ds(pl.multiple_of(early + plane * span + t * TILE, TILE), TILE)
                high_ref[k, at, :] = high
                low_ref[k, at, :] = low

            first = pl.multiple_of(begin + t * TILE, TILE)
            outer_tile(edge, inputs, rows, turn_ref[pl.ds(first, TILE), :], tmp_ref, store)

    for copy in copies[:first]:
        copy.wait()
    lower = lax.broadcasted_iota(jnp.int32, (INNER, LANES), 1) < COLS
    sum_ref[...] = jnp.zeros_like(sum_ref)

    @pl.loop(0, acc_ref.shape[0], unroll=2)
    def _(step):
        total = acc_ref[step]
        part = 0.0
        for block in range(GROUP // 8):
            ks = [GROUP * step + 8 * block + n for n in range(8)]
            if last:
                out = sums_ref[step] + matmul(table_ref[...], jnp.concatenate([e_ref[k] for k in ks], axis=1))
            else:
                table = jnp.concatenate([th_ref[...], th_ref[...], tl_ref[...]], axis=1)
                high = jnp.concatenate([high_ref[k] for k in ks], axis=1)
                low = jnp.concatenate([low_ref[k] for k in ks], axis=1)
                out = matmul(table, jnp.concatenate([high, low, high], axis=0))
            xs = []
            for pair in range(8 // 2):
                x = 0.0
                for plane in range(2):
                    z = out[plane * INNER : (plane + 1) * INNER, 2 * pair * LANES : 2 * (pair + 1) * LANES]
                    a, b = z[:, :LANES], z[:, LANES:]
                    x += jnp.where(lower, a, b) * pltpu.roll(jnp.where(lower, b, a), COLS, 1)
                xs.append(jnp.concatenate(split(x), axis=1))
            x = jnp.concatenate(xs, axis=0)
            r = matmul(x, cw_ref[...])
            r = r[:, :LANES] + r[:, LANES:]
            for pair in range(8 // 2):
                turn = 2 * hypers * (8 // 2 * block + pair)
                one = r[pair * INNER : (pair + 1) * INNER]
                total += pltpu.roll(one, turn, 1) if turn else one
            for quad in range(8 // 4):
                part += matmul(
                    rr_ref[GROUP // 4 * step + 8 // 4 * block + quad],
                    x[2 * quad * INNER : 2 * (quad + 1) * INNER],
                )
        sum_ref[...] += part
        acc_ref[step] = total

    t = sum_ref[...]
    both = []
    for n in range(2):
        at = 2 * n * hypers
        both.append(
            t[at : at + hypers, :LANES] + t[at + hypers : at + 2 * hypers, :LANES] + t[at : at + hypers, LANES:]
        )
    col = both[0] + pltpu.roll(both[1], COLS, 1)
    if not last:
        col_ref[...] = col
        return

    for copy in copies[first:]:
        copy.wait()
    outer = fin_ref.shape[1] * 2 // hypers
    acc = jnp.concatenate([acc_ref[n] for n in range(acc_ref.shape[0])], axis=1)
    parts = split(acc)
    ahead = sum(matmul(part, ahead_ref[...]) for part in parts)
    behind = sum(matmul(part, behind_ref[...]) for part in parts)
    column = lax.broadcasted_iota(jnp.int32, behind.shape, 1)
    behind = jnp.where(column % outer == 0, pltpu.roll(behind, INNER - 1, 0), behind)
    row = lax.broadcasted_iota(jnp.int32, (INNER, INNER), 0)
    column = lax.broadcasted_iota(jnp.int32, (INNER, INNER), 1)
    flip = jnp.where(row + column == INNER - 1, 1.0, 0.0).astype(jnp.bfloat16)
    fin_ref[...] = ahead + sum(matmul(flip, part) for part in split(behind))

    mine = before_ref[...] + keep_ref[0] * col + keep_ref[1] * pltpu.roll(col, COLS, 1)
    depth = INNER // members
    groups = fin_ref.shape[1] // LANES
    for d in range(members):
        for n in range(groups):
            pay_ref[d, n * depth : (n + 1) * depth, :] = fin_ref[
                d * depth : (d + 1) * depth, n * LANES : (n + 1) * LANES
            ]
        pay_ref[d, groups * depth :, :] = mine


def inner_stage(pieces, turns, begin, edge, early, table, rr, cw, acc, closing):
    shards = len(pieces)
    _, depth, span, _ = pieces[0].shape
    outer = shards * depth
    hypers = 2 * LANES // (2 * GROUP)
    whole = lambda a: pl.BlockSpec(a.shape, lambda i: (0,) * len(a.shape))
    scratch = []
    members = 0
    if closing:
        orders, before, keep, members = closing
        extra, small = list(orders), [before, keep]
        table = [three_table(table, begin, span)]
        early = [early]
        held = [pltpu.VMEM((outer, 6 * span, LANES), jnp.bfloat16), pltpu.VMEM(early[0].shape, jnp.float32)]
        lines = hypers // 2 * outer // LANES * (INNER // members) + hypers
        out_shape = [jax.ShapeDtypeStruct((members, lines, LANES), jnp.float32)]
        scratch = [
            pltpu.VMEM(acc.shape, jnp.float32),
            pltpu.VMEM((INNER, hypers // 2 * outer), jnp.float32),
            *[pltpu.VMEM(o.shape, o.dtype) for o in orders],
        ]
    else:
        extra, small = [], []
        early = [f.reshape(outer, -1, LANES) for f in early]
        held = [pltpu.VMEM((outer, 2 * INNER, LANES), jnp.bfloat16)] * 2
        out_shape = [
            jax.ShapeDtypeStruct(acc.shape, jnp.float32),
            jax.ShapeDtypeStruct((hypers, LANES), jnp.float32),
        ]
    return pl.pallas_call(
        functools.partial(inner_kernel, shards, begin, edge, members),
        grid=(1,),
        in_specs=[whole(a) for a in (*pieces, turns, *table, cw)]
        + [pl.BlockSpec(memory_space=pl.ANY)] * (len(early) + 2 + len(extra))
        + [whole(a) for a in small],
        out_specs=[whole(a) for a in out_shape],
        out_shape=out_shape,
        scratch_shapes=scratch
        + [
            *held,
            pltpu.VMEM((shards, 2, depth, TILE, LANES), jnp.float32),
            pltpu.VMEM((4 * hypers, 2 * LANES), jnp.float32),
            pltpu.VMEM(rr.shape, rr.dtype),
            pltpu.SemaphoreType.DMA((len(early) + 2 + len(extra),)),
        ],
        compiler_params=pltpu.CompilerParams(vmem_limit_bytes=VMEM_LIMIT),
        cost_estimate=pl.CostEstimate(
            flops=2 * 3 * 4 * outer * INNER * INNER * LANES,
            bytes_accessed=8 * outer * INNER * LANES,
            transcendentals=0,
        ),
        name="inner",
    )(*pieces, turns, *table, cw, *early, rr, acc, *extra, *small)


def orders_kernel(ahead_ref, behind_ref):
    lanes, width = ahead_ref.shape
    hypers = LANES // GROUP
    outer = lanes // hypers
    row = lax.broadcasted_iota(jnp.int32, (lanes, width), 0)
    column = lax.broadcasted_iota(jnp.int32, (lanes, width), 1)
    k, h = column % outer, column // outer
    one = lambda hit: jnp.where(hit, 1.0, 0.0).astype(jnp.bfloat16)
    ahead_ref[...] = one(row == hypers * k + h)
    behind_ref[...] = one(row == hypers * ((outer - k) % outer) + hypers // 2 + h)


def output_orders(outer, hyper):
    shape = jax.ShapeDtypeStruct((2 * hyper * outer, hyper * outer), jnp.bfloat16)
    return pl.pallas_call(
        orders_kernel,
        out_shape=[shape, shape],
        compiler_params=pltpu.CompilerParams(vmem_limit_bytes=VMEM_LIMIT),
        cost_estimate=pl.CostEstimate(flops=0, bytes_accessed=4 * shape.size, transcendentals=0),
        name="orders",
    )()


def local(probes, solves, row_spectra, col_spectra):
    shards = lax.axis_size("row")
    groups = lax.axis_size("grp")
    position = lax.axis_index("row")
    local_probes, rows, second_len = probes.shape
    hyper, first_len = row_spectra.shape
    half_len = second_len // 2
    block = half_len // shards
    chunks = block // COLS
    outer = first_len // INNER
    scale = 1.0 / (local_probes * groups * first_len * second_len)

    tables = column_tables(second_len, shards, chunks)
    where_am_i = position.astype(jnp.int32).reshape(1)

    k = jnp.arange(outer, dtype=jnp.int32)
    count = k[:, None] * jnp.arange(INNER, dtype=jnp.int32)[None, :] + (k % shards * position * rows)[:, None]
    phase = (count % first_len).astype(jnp.float32) * (2.0 * math.pi / first_len)
    turns = jnp.concatenate([jnp.cos(phase), -jnp.sin(phase)], axis=0).T

    forward = row_spectra.reshape(hyper, INNER, outer).transpose(0, 2, 1) * scale
    i = np.arange(INNER)
    exact = functools.partial(jnp.einsum, precision=lax.Precision.HIGHEST)
    turned = exact("mn,hnk->hmk", np.eye(outer, dtype=np.float32)[-np.arange(outer) % outer], forward)
    mirror = jnp.concatenate(
        [
            exact("hmk,ka->hma", turned[:, :1], np.eye(INNER, dtype=np.float32)[-i % INNER]),
            exact("hmk,ka->hma", turned[:, 1:], np.eye(INNER, dtype=np.float32)[INNER - 1 - i]),
        ],
        axis=1,
    )
    rr = jnp.concatenate([forward, mirror], axis=0)
    rr = rr.reshape(2 * hyper, outer // 4, 2, 2, INNER).transpose(1, 3, 0, 2, 4)
    rr = jnp.stack(split_plain(rr), axis=2).reshape(outer // 4, 8 * hyper, 2 * INNER)

    start = position * block
    ahead = lax.dynamic_slice_in_dim(col_spectra, start, block, 1)
    reverse = jnp.concatenate(
        [col_spectra[:, half_len : half_len + 1], col_spectra[:, :half_len:-1]], axis=1
    )
    behind = lax.dynamic_slice_in_dim(reverse, start, block, 1)
    edge_column = jnp.logical_and(position == 0, jnp.arange(block) == 0)
    both = jnp.concatenate([ahead, behind], axis=0) * scale
    main = jnp.where(edge_column, 0.0, both).reshape(2 * hyper, chunks, COLS).transpose(1, 2, 0)
    rim = jnp.where(position == 0, both[:, 0].reshape(2, hyper), 0.0)
    rim = jnp.pad(rim, ((0, COLS - 2), (0, hyper)))
    cw = jnp.concatenate([main, rim[None]], axis=0)
    cw = jnp.concatenate(
        [
            jnp.pad(cw, ((0, 0), (0, 0), (0, LANES - 2 * hyper))),
            jnp.pad(cw, ((0, 0), (0, 0), (2 * hyper, LANES - 4 * hyper))),
        ],
        axis=1,
    )
    high, low = split_plain(cw)
    cw = jnp.concatenate(
        [jnp.concatenate([high, low], axis=2), jnp.concatenate([high, jnp.zeros_like(low)], axis=2)], axis=1
    )
    orders = output_orders(outer, hyper)

    members = groups * shards
    order = [shards // 2, shards // 4, 3 * shards // 4, 3]
    order += [m for m in range(1, shards) if m not in order] + [0]
    moved = []

    def send(n, c, begin, span, after=None):
        fields = probes[n], solves[n]
        if after is not None:
            *fields, _ = lax.optimization_barrier((*fields, after))
        sent = {}
        for ahead in (order,) if moved else (order[:2], order[2:4], order[4:]):
            out = columns(*fields, [t[c] for t in tables], where_am_i, shards, ahead, begin, span)
            sent.update(zip(ahead, out))
        for m in order[:-1]:
            sent[m] = lax.ppermute(sent[m], "row", [(i, (i + m) % shards) for i in range(shards)])
        moved.append([sent[m] for m in range(shards)])

    todo = [
        (n, c, sum(pieces_of(c)[:at]), span)
        for n in range(local_probes)
        for c in range(chunks)
        for at, span in enumerate(pieces_of(c))
    ]
    early_sends = todo if len(todo) < 4 else todo[:-1]
    for piece in early_sends:
        send(*piece)
    acc = jnp.zeros((outer // GROUP, INNER, LANES), jnp.float32)
    col_parts = [0.0] * chunks
    rim_col = 0.0
    slots = np.arange(LANES)
    for n in range(local_probes):
        for c in range(chunks):
            spans = pieces_of(c)
            table = inner_table(spans)
            at = 2 * (n * chunks + c)
            if at + 2 > len(moved):
                send(*todo[-1], after=col)
            first, second = moved[at : at + 2]
            for edge in (True, False) if c == 0 else (False,):
                closing = None
                if not (n == local_probes - 1 and c == chunks - 1 and not edge):
                    early = outer_stage(first, turns, 0, edge)
                else:
                    early = early_stage(first, turns, 0, table)
                    rim_first = jnp.concatenate([rim_col[:hyper, 0], rim_col[:hyper, 1]])[:, None]
                    rim_first = jnp.where(jnp.logical_and(position == 0, slots == 0), rim_first, 0.0)
                    clear = jnp.where(jnp.logical_and(position == 0, slots == 0), 0.0, 1.0)
                    mine = jnp.pad(
                        jnp.concatenate(
                            [jnp.zeros((2 * hyper, 0), jnp.float32)]
                            + [
                                jnp.broadcast_to(part, (2 * hyper, LANES))[:, :COLS] + jnp.zeros((2 * hyper, COLS))
                                for part in col_parts
                            ],
                            axis=1,
                        ),
                        ((0, 0), (0, LANES - chunks * COLS)),
                    )
                    before = mine * clear + rim_first
                    keep = jnp.stack(
                        [jnp.where((slots // COLS == c) & (c == k), clear, 0.0) for k in range(2)]
                    )
                    keep = jnp.broadcast_to(keep[:, None], (2, 2 * hyper, LANES))
                    closing = (orders, before, keep, members)
                out = inner_stage(
                    second, turns, spans[0], edge, early, table, rr, cw[chunks if edge else c], acc, closing
                )
                if closing:
                    (payload,) = out
                elif edge:
                    acc, col = out
                    rim_col = rim_col + col
                else:
                    acc, col = out
                    col_parts[c] = col_parts[c] + col

    got = lax.all_to_all(payload, ("grp", "row"), split_axis=0, concat_axis=0, tiled=True)
    depth = INNER // members
    lines = hyper * outer // LANES
    row_sum = jnp.sum(got[:, : lines * depth], axis=0).reshape(lines, depth, hyper // lines, outer)
    row_traces = row_sum.transpose(0, 2, 1, 3).reshape(hyper, depth * outer)
    col_all = jnp.sum(got[:, lines * depth :, :block].reshape(groups, shards, 2, hyper, block), axis=0)
    col_all = col_all.transpose(1, 2, 0, 3).reshape(2, hyper, half_len)
    col_traces = jnp.concatenate([col_all[0], col_all[1, :, :1], col_all[1, :, :0:-1]], axis=1)
    return (row_traces, col_traces)


def solution(mesh):
    placed = (P("grp", "row", None), P("grp", "row", None), P(), P())
    return jax.shard_map(
        local, mesh=mesh, in_specs=placed, out_specs=(P(None, ("grp", "row")), P()), check_vma=False
    )
```
